128 devices in a mesh: rep: 16 (over y, x_hi, core), fsdp: 8 (over x_lo, z).
Axes of the slice: x: 4 (x_hi: 2, x_lo: 2; x = x_hi * 2 + x_lo), y: 4, z: 4, core: 2. Of those that a mesh axis runs over, the one named last changes fastest.
Arguments:
- replica_inner_weight: bfloat16 [16, 1024, 16384], P('rep', 'fsdp'), may hold values from -30 to 30
- outer_weights: float32 [1024, 16384], P('fsdp'), may hold values from -6 to 6
- momentum: float32 [1024, 16384], P('fsdp', 'rep'), may hold values from -4 to 4
- exponents: int32 [16, 1024, 128], P('rep', 'fsdp'), may hold values from 0 to 2
- levels: int32 [16], replicated, may hold values from -60 to 60, as said below
Outputs:
- inner_next: bfloat16 [16, 1024, 16384], P('rep', 'fsdp')
- momentum_next: float32 [1024, 16384], P('fsdp', 'rep')
- outer_next: float32 [1024, 16384], P('fsdp', 'rep')
The draws below stay inside these ranges and needn't reach their ends.
Inputs may be any that keep to these rules, and one draw needn't show every extreme that they name: `levels`: 16 distinct values, half of them negative and half positive, ascending.
All inputs are finite; a program needn't handle non-finite values. Where the reference program divides by a largest or mean magnitude, that divisor is 1e-20 or more.
Results may differ from the reference program's by a relative error of at most 0.0085.
Values may be sent and summed in bfloat16 or wider, within the bound.
No kernel may reach another device: no remote copies, remote signals or barrier semaphores. Data moves between devices by JAX's collectives and lax.ppermute only.
A program may use at most 128 MiB of HBM per device.

```python
import jax
import jax.numpy as jnp
from jax import lax

D = 16384
BLOCK = 128
NLEV = 16
ROWS = 1024
REPS = 16


def draw_levels(key, part):
    base_key = jax.random.fold_in(key, 11)
    first_key, second_key = jax.random.split(base_key)
    negative = jax.random.permutation(first_key, 60)[:NLEV // 2] + 1
    positive = jax.random.permutation(second_key, 60)[:NLEV // 2] + 1
    values = jnp.concatenate([-negative, positive])
    return jnp.sort(values).astype(jnp.int32)


def weight_fields(key):
    base_key = jax.random.fold_in(key, 23)
    outer_key, noise_key = jax.random.split(base_key, 2)
    outer_field = jnp.clip(jax.random.normal(outer_key, (ROWS, D), jnp.float32), -6.0, 6.0)
    noise = jnp.clip(jax.random.normal(noise_key, (REPS, ROWS, D), jnp.float32), -6.0, 6.0)
    position = jnp.arange(ROWS, dtype=jnp.float32) / jnp.float32(max(ROWS - 1, 1))
    column_place = jnp.arange(D, dtype=jnp.float32) / jnp.float32(max(D - 1, 1))
    row_scale = 0.12 * jnp.exp(position * jnp.log(8.0))
    column_scale = 0.5 * jnp.exp(column_place * jnp.log(4.0))
    spread = row_scale[:, None] * column_scale[None, :]
    inner_field = jnp.clip(outer_field[None] - spread[None] * noise, -30.0, 30.0)
    return (outer_field, inner_field)


def draw_outer_weights(key, part):
    return weight_fields(key)[0].astype(jnp.float32)


def draw_replica_inner_weight(key, part):
    return weight_fields(key)[1].astype(jnp.bfloat16)


def touch_ends(array, rng, smallest, high):
    extent = array.shape
    spot = [jax.random.randint(jax.random.fold_in(rng, axis), (), 0, extent[axis]) for axis in range(len(extent))]
    array = array.at[tuple(spot)].set(smallest)
    longest = extent.index(max(extent))
    spot[longest] = (spot[longest] + 1) % extent[longest]
    return array.at[tuple(spot)].set(high)


def steps_of(rng, shape, shards, least, largest):
    loudness, own = 1.0, jax.random.fold_in(rng, 6)
    for dim, shards_of in shards:
        steps = jnp.exp(jax.random.uniform(jax.random.fold_in(own, dim), (shards_of,), jnp.float32, least / len(shards), largest / len(shards)))
        loudness = loudness * jnp.repeat(steps, shape[dim] // shards_of).reshape([-1 if axis == dim else 1 for axis in range(len(shape))])
    return loudness


def scatter_about(key, shape, deviation, most, cuts=(), kind=jnp.bfloat16):
    entries = jax.random.normal(key, shape, jnp.float32) * deviation
    if len(cuts) > 0:
        entries = steps_of(key, shape, cuts, -0.22, 0.18) * entries
    return jnp.clip(entries, min=-most, max=most).astype(kind)


def setup_inputs(seed: int = 0) -> dict:
    arg_keys = jax.random.split(jax.random.key(seed), 6)
    replica_inner_weight = draw_replica_inner_weight(jax.random.fold_in(arg_keys[5], 71), 0)
    outer_weights = draw_outer_weights(jax.random.fold_in(arg_keys[5], 71), 0)
    momentum = scatter_about(arg_keys[2], (ROWS, D), 0.3, 4.0, ((0, 8), (1, 16)), jnp.float32)
    exponents = touch_ends(jax.random.randint(arg_keys[3], (REPS, ROWS, D // BLOCK), 0, 3), jax.random.fold_in(arg_keys[3], 1), 0, 2).astype(jnp.int32)
    levels = draw_levels(jax.random.fold_in(arg_keys[5], 71), 0)
    return {"replica_inner_weight": replica_inner_weight, "outer_weights": outer_weights, "momentum": momentum, "exponents": exponents, "levels": levels}


softness_factor = 0.02
clip_rms = 0.1
outer_rate = 0.7
outer_mu = 0.9
mix_rate = 0.5

def encode_grad(pseudo_grad, exponents, levels):
    quantize_grid_points = levels.astype(jnp.float32) / jnp.max(jnp.abs(levels)).astype(jnp.float32)
    block_scale = jnp.exp2(exponents.astype(jnp.float32))[..., None]
    row_count = pseudo_grad.shape[0]
    rescaled_gradient = pseudo_grad.reshape(row_count, exponents.shape[-1], -1) / block_scale
    closest_grid_level = (rescaled_gradient - quantize_grid_points[0]) ** 2
    for grid_level_index in range(1, NLEV):
        closest_grid_level = jnp.minimum(closest_grid_level, (rescaled_gradient - quantize_grid_points[grid_level_index]) ** 2)
    weighted = jnp.zeros_like(rescaled_gradient)
    weights_sum = jnp.zeros_like(rescaled_gradient)
    for grid_level_index in range(NLEV):
        current_weight = jnp.exp(-((rescaled_gradient - quantize_grid_points[grid_level_index]) ** 2 - closest_grid_level) / softness_factor)
        weighted = weighted + current_weight * quantize_grid_points[grid_level_index]
        weights_sum = weights_sum + current_weight
    coded = block_scale * weighted / weights_sum
    return coded.reshape(row_count, -1).astype(jnp.bfloat16)

def reference(replica_inner_weight, outer_weights, momentum, exponents, levels):
    replicas = replica_inner_weight.shape[0]

    def accumulate(running, items):
        inner_one, expo_one = items
        coded = encode_grad(outer_weights - inner_one.astype(jnp.float32), expo_one, levels)
        return (running + coded.astype(jnp.float32), None)
    running = lax.scan(accumulate, jnp.zeros(outer_weights.shape, jnp.float32), (replica_inner_weight, exponents))[0]
    mean_grad = running / jnp.float32(replicas)
    mean_square = jnp.sum(mean_grad * mean_grad) / jnp.float32(mean_grad.size)
    clip = jnp.minimum(jnp.float32(1.0), clip_rms / jnp.sqrt(mean_square + 1e-06))
    grad = clip * mean_grad
    momentum_next = outer_mu * momentum + grad
    outer_next = outer_weights - outer_rate * (grad + outer_mu * momentum_next)
    outer_half = outer_next.astype(jnp.bfloat16)

    def blend(inner_one):
        return (mix_rate * outer_half.astype(jnp.float32) + (1.0 - mix_rate) * inner_one.astype(jnp.float32)).astype(jnp.bfloat16)
    inner_next = lax.map(blend, replica_inner_weight)
    return (inner_next, momentum_next, outer_next)
```

```python
import math

import jax
import jax.numpy as jnp
from jax import lax
from jax.experimental import pallas as pl
from jax.experimental.pallas import tpu as pltpu
from jax.sharding import Mesh
from jax.sharding import PartitionSpec as P

NLEV = 16
LANES = 128
REP = ("rep_0", "rep_1", "rep_2")
CHIPS = ("rep_0", "rep_1")
CORE = "rep_2"
FSDP = ("fsdp_0", "fsdp_1")

softness_factor = 0.02
clip_rms = 0.1
outer_rate = 0.7
outer_mu = 0.9
mix_rate = 0.5

STRETCH = math.sqrt(1.0 / (softness_factor * math.log(2.0)))
WIDTHS = (512, 512)
GROUP = 256
TILE = 64


def prepare(levels):
    def body(lev, grid_ref, sum_ref):
        top = jnp.abs(lev[0])
        for k in range(1, NLEV):
            top = jnp.maximum(top, jnp.abs(lev[k]))
        top = jnp.full((8, LANES), top, jnp.int32).astype(jnp.float32)
        row = lax.broadcasted_iota(jnp.int32, (LANES, 2 * LANES), 0)
        col = lax.broadcasted_iota(jnp.int32, (LANES, 2 * LANES), 1)
        for k in range(NLEV):
            lk = jnp.full((8, LANES), lev[k], jnp.int32).astype(jnp.float32)
            grid_ref[k] = lk / top * STRETCH
            level = jnp.full((LANES, 2 * LANES), lev[k], jnp.int32)
            one = jnp.where(row == col, 1, jnp.where(row + LANES == col, level, 0))
            sum_ref[k * LANES:(k + 1) * LANES, :] = one.astype(jnp.float32).astype(jnp.bfloat16)
        grid_ref[NLEV] = 1.0 / top

    return pl.pallas_call(
        body,
        in_specs=[pl.BlockSpec(memory_space=pltpu.SMEM)],
        out_shape=(
            jax.ShapeDtypeStruct((NLEV + 1, 8, LANES), jnp.float32),
            jax.ShapeDtypeStruct((NLEV * LANES, 2 * LANES), jnp.bfloat16),
        ),
        name="prepare",
    )(levels)


def encode(where, grid, summing, outer, inner, exponents, width, received=None):
    rows = outer.shape[0]
    owners = 8
    per_step = max(1, 1024 // width)
    steps = owners // per_step
    blocks = width // LANES
    group_blocks = GROUP // rows
    groups = [(a, g) for a in range(per_step) for g in range(blocks // group_blocks)]

    def body(*refs):
        idx, grid_ref, sum_ref, exp_ref = refs[:4]
        outer_refs = refs[4:4 + per_step]
        inner_refs = refs[4 + per_step:4 + 2 * per_step]
        rest = refs[4 + 2 * per_step:]
        recv_ref = rest[0] if received is not None else None
        out_ref = rest[-1]
        step = pl.program_id(0)
        lanes = lax.broadcasted_iota(jnp.int32, (TILE, LANES), 1)

        def points(k):
            return jnp.broadcast_to(grid_ref[k, 0:1, :], (TILE, LANES))

        def scoped(w0, w1, s0, s1):
            weights = (w0, w1)
            scales = (s0, s1)

            def weigh(which, slot):
                a, g = which
                unit = (idx[0] + (step * per_step + a) * idx[1]) * blocks
                for jj in range(group_blocks):
                    j = g * group_blocks + jj
                    for r in range(0, rows, TILE):
                        ex = exp_ref[0, r:r + TILE, :].astype(jnp.float32)
                        ex = jnp.sum(jnp.where(lanes == unit + j, ex, 0.0), axis=1, keepdims=True)
                        ex = jnp.broadcast_to(ex, (TILE, LANES))
                        m = jj * rows + r
                        scales[slot][m:m + TILE, :] = jnp.exp2(ex) * points(NLEV)
                        cols = slice(j * LANES, (j + 1) * LANES)
                        pseudo = outer_refs[a][r:r + TILE, cols] - inner_refs[a][0, r:r + TILE, cols].astype(jnp.float32)
                        v = pseudo * (jnp.exp2(-ex) * STRETCH)
                        near = jnp.minimum(jnp.maximum(v, points(0)), points(NLEV - 1))
                        far = (v + v) - near
                        for k in range(NLEV):
                            e = (points(k) - near) * (far - points(k))
                            weights[slot][m:m + TILE, k * LANES:(k + 1) * LANES] = jnp.exp2(e).astype(jnp.bfloat16)

            def average(which, slot):
                a, g = which
                sums = jnp.dot(weights[slot][...], sum_ref[...], preferred_element_type=jnp.float32)
                coded = sums[:, LANES:] / sums[:, :LANES] * scales[slot][...]
                for jj in range(group_blocks):
                    cols = slice((g * group_blocks + jj) * LANES, (g * group_blocks + jj + 1) * LANES)
                    piece = coded[jj * rows:(jj + 1) * rows]
                    if recv_ref is not None:
                        piece = piece + recv_ref[a, :, cols].astype(jnp.float32)
                    out_ref[a, :, cols] = piece.astype(jnp.bfloat16)

            weigh(groups[0], 0)
            for n in range(1, len(groups)):
                weigh(groups[n], n % 2)
                average(groups[n - 1], (n - 1) % 2)
            average(groups[-1], (len(groups) - 1) % 2)

        pl.run_scoped(
            scoped,
            pltpu.VMEM((GROUP, NLEV * LANES), jnp.bfloat16),
            pltpu.VMEM((GROUP, NLEV * LANES), jnp.bfloat16),
            pltpu.VMEM((GROUP, LANES), jnp.float32),
            pltpu.VMEM((GROUP, LANES), jnp.float32),
        )

    def unit_of(a):
        return lambda s, idx: idx[0] + (s * per_step + a) * idx[1]

    in_specs = [
        pl.BlockSpec((NLEV + 1, 8, LANES), lambda s, idx: (0, 0, 0)),
        pl.BlockSpec((NLEV * LANES, 2 * LANES), lambda s, idx: (0, 0)),
        pl.BlockSpec((1, rows, LANES), lambda s, idx: (0, 0, 0)),
    ]
    in_specs += [pl.BlockSpec((rows, width), lambda s, idx, f=unit_of(a): (0, f(s, idx))) for a in range(per_step)]
    in_specs += [pl.BlockSpec((1, rows, width), lambda s, idx, f=unit_of(a): (0, 0, f(s, idx))) for a in range(per_step)]
    piece = pl.BlockSpec((per_step, rows, width), lambda s, idx: (s, 0, 0))
    args = [where, grid, summing, exponents] + [outer] * per_step + [inner] * per_step
    if received is not None:
        in_specs.append(piece)
        args.append(received)
    return pl.pallas_call(
        body,
        grid_spec=pltpu.PrefetchScalarGridSpec(
            num_scalar_prefetch=1, grid=(steps,), in_specs=in_specs, out_specs=piece
        ),
        out_shape=jax.ShapeDtypeStruct((owners, rows, width), jnp.bfloat16),
        cost_estimate=pl.CostEstimate(
            flops=int(owners * rows * width * 130), transcendentals=0,
            bytes_accessed=int(owners * rows * width * 8),
        ),
        name="encode_keep" if received is not None else "encode_send",
    )(*args)


def owners_mean(pieces, replicas):
    senders, rows, width = pieces.shape

    def body(in_ref, mean_ref, copies_ref, squares_ref):
        total = in_ref[0].astype(jnp.float32)
        for s in range(1, senders):
            total = total + in_ref[s].astype(jnp.float32)
        mean = total / replicas
        mean_ref[...] = mean
        half = mean.astype(jnp.bfloat16)
        for s in range(senders):
            copies_ref[s] = half
        sq = mean * mean
        acc = sq[0:8, 0:LANES]
        for r in range(0, rows, 8):
            for c in range(0, width, LANES):
                if r or c:
                    acc = acc + sq[r:r + 8, c:c + LANES]
        squares_ref[...] = acc

    return pl.pallas_call(
        body,
        out_shape=(
            jax.ShapeDtypeStruct((rows, width), jnp.float32),
            jax.ShapeDtypeStruct((senders, rows, width), jnp.bfloat16),
            jax.ShapeDtypeStruct((8, LANES), jnp.float32),
        ),
        name="owners_mean",
    )(pieces)


def blend(where, squares, entries, outer, inner, momenta, means, partial):
    rows, columns = outer.shape
    owners, _, width = momenta.shape
    spans = [m.shape[2] for m in means]

    def body(idx, sq_ref, outer_ref, inner_ref, mom_ref, *rest):
        mean_refs = rest[:len(spans)]
        out_ref = rest[-1]
        mean_square = jnp.sum(sq_ref[...]) / entries
        clip = jnp.minimum(
            1.0, clip_rms / jnp.sqrt(jnp.full((8, LANES), mean_square, jnp.float32) + 1e-06)
        )[0:1, 0:1]
        at = 0
        for span, ref in zip(spans, mean_refs):
            cols = slice(at, at + span)
            grad = clip * ref[0].astype(jnp.float32)
            momentum_next = outer_mu * mom_ref[0, :, cols].astype(jnp.float32) + grad
            outer_next = outer_ref[:, cols] - outer_rate * (grad + outer_mu * momentum_next)
            half = outer_next.astype(jnp.bfloat16).astype(jnp.float32)
            mixed = mix_rate * half + (1.0 - mix_rate) * inner_ref[0, :, cols].astype(jnp.float32)
            out_ref[0, :, cols] = mixed.astype(jnp.bfloat16)
            at += span

    def unit(d, idx):
        return idx[0] + d * idx[1]

    in_specs = [
        pl.BlockSpec((8, LANES), lambda d, idx: (0, 0)),
        pl.BlockSpec((rows, width), lambda d, idx: (0, unit(d, idx))),
        pl.BlockSpec((1, rows, width), lambda d, idx: (0, 0, unit(d, idx))),
        pl.BlockSpec((1, rows, width), lambda d, idx: (d, 0, 0)),
    ]
    in_specs += [pl.BlockSpec((1, rows, span), lambda d, idx: (d, 0, 0)) for span in spans]
    args = [where, squares, outer, inner, momenta, *means]
    aliases = {}
    if partial is not None:
        in_specs.append(pl.BlockSpec(memory_space=pl.ANY))
        aliases = {len(args): 0}
        args.append(partial)
    return pl.pallas_call(
        body,
        grid_spec=pltpu.PrefetchScalarGridSpec(
            num_scalar_prefetch=1, grid=(owners,), in_specs=in_specs,
            out_specs=pl.BlockSpec((1, rows, width), lambda d, idx: (0, 0, unit(d, idx))),
        ),
        out_shape=jax.ShapeDtypeStruct((1, rows, columns), jnp.bfloat16),
        input_output_aliases=aliases,
        name="blend",
    )(*args)


def swap(array):
    return lax.ppermute(array, CORE, [(0, 1), (1, 0)])


def exchange(array, axes):
    return lax.all_to_all(array, axes, 0, 0, tiled=False)


def per_device(replica_inner_weight, outer_weights, momentum, exponents, levels):
    replicas = lax.axis_size(REP)
    rows, columns = outer_weights.shape
    entries = rows * lax.axis_size(FSDP) * columns
    width = momentum.shape[1]
    chips = lax.axis_size(CHIPS)
    core = lax.axis_index(CORE)
    start = lax.axis_index(REP) * width

    grid, summing = prepare(levels)
    own_momenta = exchange(
        jnp.broadcast_to(momentum.astype(jnp.bfloat16)[None], (chips, rows, width)), CHIPS
    )

    starts = [sum(WIDTHS[:i]) for i in range(len(WIDTHS))]

    def place(which, at, span):
        return jnp.stack([which * (width // span) + at // span, jnp.int32(2 * (width // span))]).astype(jnp.int32)

    def code(which, i, received=None):
        return encode(
            place(which, starts[i], WIDTHS[i]), grid, summing, outer_weights, replica_inner_weight,
            exponents, WIDTHS[i], received,
        )

    received = [swap(code(1 - core, i)) for i in range(len(WIDTHS))]
    received[-1], own_momenta = lax.optimization_barrier((received[-1], own_momenta))
    means, gathered, squares = [], [], []
    for i in range(len(WIDTHS)):
        pieces = exchange(code(core, i, received[i]), CHIPS)
        mean, copies, square = owners_mean(pieces, float(replicas))
        means.append(mean)
        gathered.append(exchange(copies, CHIPS))
        squares.append(square)
    square = sum(squares[1:], squares[0])
    square = jnp.sum(exchange(jnp.broadcast_to(square[None], (8, 8, LANES)), FSDP), axis=0)
    square = jnp.sum(exchange(jnp.broadcast_to(square[None], (chips, 8, LANES)), CHIPS), axis=0)
    square = square + swap(square)
    other = [swap(g) for g in gathered]
    other_momenta = swap(own_momenta)

    unit = place(core, 0, width)
    inner_next = blend(
        unit, square, float(entries), outer_weights, replica_inner_weight, own_momenta, gathered, None
    )
    unit = place(1 - core, 0, width)
    inner_next = blend(
        unit, square, float(entries), outer_weights, replica_inner_weight, other_momenta, other, inner_next
    )
    mean_grad = jnp.concatenate(means, axis=1)
    clip = jnp.minimum(
        jnp.float32(1.0), clip_rms / jnp.sqrt(jnp.sum(square) / jnp.float32(entries) + 1e-06)
    )
    grad = clip * mean_grad
    momentum_next = outer_mu * momentum + grad
    outer_piece = lax.dynamic_slice_in_dim(outer_weights, start, width, 1)
    outer_next = outer_piece - outer_rate * (grad + outer_mu * momentum_next)
    return (inner_next, momentum_next, outer_next)


def solution(mesh):
    torus = Mesh(
        mesh.devices.reshape(4, 2, 2, 2, 4), ("rep_0", "rep_1", "rep_2", "fsdp_0", "fsdp_1")
    )
    placed = (P(REP, FSDP, None), P(FSDP, None), P(FSDP, REP), P(REP, FSDP, None), P())
    return jax.shard_map(
        per_device,
        mesh=torus,
        in_specs=placed,
        out_specs=(P(REP, FSDP, None), P(FSDP, REP), P(FSDP, REP)),
        check_vma=False,
    )
```

```python
import math

import jax
import jax.numpy as jnp
from jax import lax
from jax.experimental import pallas as pl
from jax.experimental.pallas import tpu as pltpu
from jax.sharding import Mesh
from jax.sharding import PartitionSpec as P

NLEV = 16
LANES = 128
REP = ("rep_0", "rep_1", "rep_2")
FSDP = ("fsdp_0", "fsdp_1")

softness_factor = 0.02
clip_rms = 0.1
outer_rate = 0.7
outer_mu = 0.9
mix_rate = 0.5

STRETCH = math.sqrt(1.0 / (softness_factor * math.log(2.0)))
GROUP = 256
ENCODE_VMEM = 24 << 20
FINISH_VMEM = 32 << 20
TILE = 64


def prepare(levels):
    def body(lev, grid_ref, sum_ref):
        top = jnp.abs(lev[0])
        for k in range(1, NLEV):
            top = jnp.maximum(top, jnp.abs(lev[k]))
        top = jnp.full((8, LANES), top, jnp.int32).astype(jnp.float32)
        row = lax.broadcasted_iota(jnp.int32, (LANES, 2 * LANES), 0)
        col = lax.broadcasted_iota(jnp.int32, (LANES, 2 * LANES), 1)
        for k in range(NLEV):
            lk = jnp.full((8, LANES), lev[k], jnp.int32).astype(jnp.float32)
            grid_ref[k] = lk / top * STRETCH
            level = jnp.full((LANES, 2 * LANES), lev[k], jnp.int32)
            one = jnp.where(row == col, 1, jnp.where(row + LANES == col, level, 0))
            sum_ref[k * LANES:(k + 1) * LANES, :] = one.astype(jnp.float32).astype(jnp.bfloat16)
        grid_ref[NLEV] = 1.0 / top

    return pl.pallas_call(
        body,
        in_specs=[pl.BlockSpec(memory_space=pltpu.SMEM)],
        compiler_params=pltpu.CompilerParams(vmem_limit_bytes=ENCODE_VMEM),
        out_shape=(
            jax.ShapeDtypeStruct((NLEV + 1, 8, LANES), jnp.float32),
            jax.ShapeDtypeStruct((NLEV * LANES, 2 * LANES), jnp.bfloat16),
        ),
        name="prepare",
    )(levels)


def unit_of(idx, piece):
    dx, dy, dc = piece
    return (((idx[0] + dy) % 4) * 2 + (idx[1] + dx) % 2) * 2 + (idx[2] + dc) % 2


def encode(idx, grid, summing, outer, inner, exponents, width, pieces, received, stacked):
    rows = outer.shape[0]
    count = len(pieces)
    steps = 2 if count > 1 else 1
    span = width // steps
    blocks = span // LANES
    group_blocks = GROUP // rows
    groups = [(p, g) for p in range(count) for g in range(blocks // group_blocks)]
    arrays = list({id(array): array for r in received for array, _ in r}.values())

    def body(*refs):
        idx, grid_ref, sum_ref, exp_ref = refs[:4]
        outer_refs = refs[4:4 + count]
        inner_refs = refs[4 + count:4 + 2 * count]
        rest = list(refs[4 + 2 * count:])
        arrived = {id(array): rest.pop(0) for array in arrays}
        recv_refs = [[arrived[id(array)] for array, _ in r] for r in received]
        out_refs = rest
        step = pl.program_id(0)
        lanes = lax.broadcasted_iota(jnp.int32, (TILE, LANES), 1)

        def points(k):
            return jnp.broadcast_to(grid_ref[k, 0:1, :], (TILE, LANES))

        def scoped(w0, w1, s0, s1):
            weights = (w0, w1)
            scales = (s0, s1)

            def weigh(which, slot):
                p, g = which
                first = (unit_of(idx, pieces[p]) * steps + step) * blocks
                for jj in range(group_blocks):
                    j = g * group_blocks + jj
                    for r in range(0, rows, TILE):
                        ex = exp_ref[0, r:r + TILE, :].astype(jnp.float32)
                        ex = jnp.sum(jnp.where(lanes == first + j, ex, 0.0), axis=1, keepdims=True)
                        ex = jnp.broadcast_to(ex, (TILE, LANES))
                        m = jj * rows + r
                        scales[slot][m:m + TILE, :] = jnp.exp2(ex) * points(NLEV)
                        cols = slice(j * LANES, (j + 1) * LANES)
                        pseudo = outer_refs[p][r:r + TILE, cols] - inner_refs[p][0, r:r + TILE, cols].astype(jnp.float32)
                        v = pseudo * (jnp.exp2(-ex) * STRETCH)
                        near = jnp.minimum(jnp.maximum(v, points(0)), points(NLEV - 1))
                        far = (v + v) - near
                        for k in range(NLEV):
                            e = (points(k) - near) * (far - points(k))
                            weights[slot][m:m + TILE, k * LANES:(k + 1) * LANES] = jnp.exp2(e).astype(jnp.bfloat16)

            def average(which, slot):
                p, g = which
                sums = jnp.dot(weights[slot][...], sum_ref[...], preferred_element_type=jnp.float32)
                coded = sums[:, LANES:] / sums[:, :LANES] * scales[slot][...]
                for jj in range(group_blocks):
                    cols = slice((g * group_blocks + jj) * LANES, (g * group_blocks + jj + 1) * LANES)
                    part = coded[jj * rows:(jj + 1) * rows]
                    cols = pl.ds(pl.multiple_of(step * span + cols.start, LANES), LANES)
                    for ref, (_, at) in zip(recv_refs[p], received[p]):
                        part = part + ref[at, :, cols].astype(jnp.float32)
                    part = part.astype(jnp.bfloat16)
                    if stacked:
                        out_refs[0][p, :, cols] = part
                    else:
                        out_refs[p][0, :, cols] = part

            weigh(groups[0], 0)
            for n in range(1, len(groups)):
                weigh(groups[n], n % 2)
                average(groups[n - 1], (n - 1) % 2)
            average(groups[-1], (len(groups) - 1) % 2)

        pl.run_scoped(
            scoped,
            pltpu.VMEM((GROUP, NLEV * LANES), jnp.bfloat16),
            pltpu.VMEM((GROUP, NLEV * LANES), jnp.bfloat16),
            pltpu.VMEM((GROUP, LANES), jnp.float32),
            pltpu.VMEM((GROUP, LANES), jnp.float32),
        )

    in_specs = [
        pl.BlockSpec((NLEV + 1, 8, LANES), lambda s, idx: (0, 0, 0)),
        pl.BlockSpec((NLEV * LANES, 2 * LANES), lambda s, idx: (0, 0)),
        pl.BlockSpec((1, rows, LANES), lambda s, idx: (0, 0, 0)),
    ]
    in_specs += [pl.BlockSpec((rows, span), lambda s, idx, p=p: (0, unit_of(idx, p) * steps + s)) for p in pieces]
    in_specs += [pl.BlockSpec((1, rows, span), lambda s, idx, p=p: (0, 0, unit_of(idx, p) * steps + s)) for p in pieces]
    args = [idx, grid, summing, exponents] + [outer] * count + [inner] * count
    whole = pl.BlockSpec(memory_space=pltpu.VMEM)
    in_specs += [whole] * len(arrays)
    args += arrays
    if stacked:
        out_specs = whole
        out_shape = jax.ShapeDtypeStruct((count, rows, width), jnp.bfloat16)
    else:
        out_specs = [whole] * count
        out_shape = [jax.ShapeDtypeStruct((1, rows, width), jnp.bfloat16)] * count
    return pl.pallas_call(
        body,
        grid_spec=pltpu.PrefetchScalarGridSpec(
            num_scalar_prefetch=1, grid=(steps,), in_specs=in_specs, out_specs=out_specs
        ),
        out_shape=out_shape,
        cost_estimate=pl.CostEstimate(
            flops=int(count * rows * width * 200), transcendentals=0,
            bytes_accessed=int(count * rows * width * 8),
        ),
        compiler_params=pltpu.CompilerParams(vmem_limit_bytes=ENCODE_VMEM),
        name="encode",
    )(*args)


def owner_mean(parts, replicas):
    _, rows, width = parts[0].shape
    count = len(parts)
    high = 16

    def body(*refs):
        in_refs = refs[:count]
        mean_ref, half_ref, squares_ref = refs[count:]
        acc = jnp.zeros((8, LANES), jnp.float32)
        for r in range(0, rows, high):
            total = in_refs[0][0, r:r + high, :].astype(jnp.float32)
            for ref in in_refs[1:]:
                total = total + ref[0, r:r + high, :].astype(jnp.float32)
            mean = total / replicas
            mean_ref[r:r + high, :] = mean
            half_ref[0, r:r + high, :] = mean.astype(jnp.bfloat16)
            sq = mean * mean
            for k in range(0, high, 8):
                for c in range(0, width, LANES):
                    acc = acc + sq[k:k + 8, c:c + LANES]
        squares_ref[...] = acc

    whole = pl.BlockSpec(memory_space=pltpu.VMEM)
    return pl.pallas_call(
        body,
        in_specs=[whole] * count,
        out_specs=(whole, whole, whole),
        compiler_params=pltpu.CompilerParams(vmem_limit_bytes=ENCODE_VMEM),
        out_shape=(
            jax.ShapeDtypeStruct((rows, width), jnp.float32),
            jax.ShapeDtypeStruct((1, rows, width), jnp.bfloat16),
            jax.ShapeDtypeStruct((8, LANES), jnp.float32),
        ),
        name="owner_mean",
    )(*parts)


def finish(idx, squares, entries, outer, inner, momentum, mean, places, means, momenta):
    rows, columns = outer.shape
    width = momentum.shape[1]
    high = 16
    count = len(places)
    arrays = list({id(array): array for array, _ in list(means) + list(momenta)}.values())

    def step_of(grad, mom, out):
        momentum_next = outer_mu * mom + grad
        return momentum_next, out - outer_rate * (grad + outer_mu * momentum_next)

    def body(idx, sq_ref, outer_ref, inner_ref, mom_ref, mean_ref, *rest):
        given = {id(array): ref for array, ref in zip(arrays, rest)}
        inner_out, mom_out, outer_out, clip_ref = rest[len(arrays):]
        span = pl.ds(pl.multiple_of(pl.program_id(0) * high, high), high)

        @pl.when(pl.program_id(0) == 0)
        def _():
            mean_square = jnp.full((8, LANES), jnp.sum(sq_ref[...]), jnp.float32) / entries
            clip_ref[...] = jnp.minimum(1.0, clip_rms / jnp.sqrt(mean_square + 1e-06))

        clip = jnp.broadcast_to(clip_ref[0:1, :], (high, LANES))
        for p in range(count):
            base = unit_of(idx, places[p]) * width
            for c in range(0, width, LANES):
                cols = pl.ds(pl.multiple_of(base + c, LANES), LANES)
                array, at = means[p]
                grad = clip * given[id(array)][at, span, c:c + LANES].astype(jnp.float32)
                array, at = momenta[p]
                _, new = step_of(grad, given[id(array)][at, span, c:c + LANES].astype(jnp.float32), outer_ref[:, cols])
                half = new.astype(jnp.bfloat16).astype(jnp.float32)
                mixed = mix_rate * half + (1.0 - mix_rate) * inner_ref[0, :, cols].astype(jnp.float32)
                inner_out[0, :, cols] = mixed.astype(jnp.bfloat16)
        base = unit_of(idx, (0, 0, 0)) * width
        for c in range(0, width, LANES):
            cols = pl.ds(pl.multiple_of(base + c, LANES), LANES)
            grad = clip * mean_ref[:, c:c + LANES]
            mom, new = step_of(grad, mom_ref[:, c:c + LANES], outer_ref[:, cols])
            mom_out[:, c:c + LANES] = mom
            outer_out[:, c:c + LANES] = new

    in_specs = [
        pl.BlockSpec((8, LANES), lambda s, idx: (0, 0)),
        pl.BlockSpec((high, columns), lambda s, idx: (s, 0)),
        pl.BlockSpec((1, high, columns), lambda s, idx: (0, s, 0)),
        pl.BlockSpec((high, width), lambda s, idx: (s, 0)),
        pl.BlockSpec((high, width), lambda s, idx: (s, 0)),
    ]
    args = [idx, squares, outer, inner, momentum, mean]
    in_specs += [pl.BlockSpec(memory_space=pltpu.VMEM)] * len(arrays)
    args += arrays
    return pl.pallas_call(
        body,
        grid_spec=pltpu.PrefetchScalarGridSpec(
            num_scalar_prefetch=1, grid=(rows // high,), in_specs=in_specs,
            out_specs=[
                pl.BlockSpec((1, high, columns), lambda s, idx: (0, s, 0)),
                pl.BlockSpec((high, width), lambda s, idx: (s, 0)),
                pl.BlockSpec((high, width), lambda s, idx: (s, 0)),
            ],
            scratch_shapes=[pltpu.VMEM((8, LANES), jnp.float32)],
        ),
        out_shape=[
            jax.ShapeDtypeStruct((1, rows, columns), jnp.bfloat16),
            jax.ShapeDtypeStruct((rows, width), jnp.float32),
            jax.ShapeDtypeStruct((rows, width), jnp.float32),
        ],
        compiler_params=pltpu.CompilerParams(vmem_limit_bytes=FINISH_VMEM),
        name="finish",
    )(*args)


def shift(array, axis, by):
    size = lax.axis_size(axis)
    return lax.ppermute(array, axis, [(i, (i + by) % size) for i in range(size)])


def add_over(array, axes):
    sizes = [lax.axis_size(axis) for axis in axes]
    total = math.prod(sizes)
    parts = [array]
    for by in range(1, total):
        moves = []
        for i in range(total):
            if len(axes) == 1:
                moves.append((i, (i + by) % total))
            else:
                moves.append((i, i ^ by))
        parts.append(lax.ppermute(array, axes, moves))
    return sum(parts[1:], parts[0])


RING, PAIR, CORE = REP
AROUND = (1, 3, 2)


def per_device(replica_inner_weight, outer_weights, momentum, exponents, levels):
    replicas = lax.axis_size(REP)
    rows, columns = outer_weights.shape
    entries = rows * lax.axis_size(FSDP) * columns
    width = momentum.shape[1]
    idx = jnp.stack([lax.axis_index(axis) for axis in REP]).astype(jnp.int32)

    grid, summing = prepare(levels)

    def code(pieces, received, stacked=False):
        return encode(
            idx, grid, summing, outer_weights, replica_inner_weight, exponents, width, pieces, received, stacked
        )

    half = momentum.astype(jnp.bfloat16)[None]
    ring = [half, None, None, None]
    for by in AROUND:
        ring[(4 - by) % 4] = shift(half, RING, by)

    order = [(1, 1), (1, 3), (1, 2), (0, 1), (0, 3), (1, 0), (0, 2), (0, 0)]
    sibling = {}

    def send(part, idx):
        pieces = [(dx, dy, 1) for dx, dy in part]
        swapped = shift(
            encode(idx, grid, summing, outer_weights, replica_inner_weight, exponents, width, pieces, [[] for _ in part], True),
            CORE, 1,
        )
        for n, place in enumerate(part):
            sibling[place] = (swapped, n)

    send(order[:4], idx)
    near_momenta = jnp.concatenate(ring, axis=0)
    near_momenta, later = lax.optimization_barrier((near_momenta, idx))
    send(order[4:], later)
    far_momenta = shift(near_momenta, PAIR, 1)

    def keep(places, more):
        return code([(dx, dy, 0) for dx, dy in places], [[sibling[p]] + [(a, 0) for a in m] for p, m in zip(places, more)])

    out1, out3, out2 = keep(order[:3], [[], [], []])
    in1, in3, in2 = shift(out1, RING, 1), shift(out3, RING, 3), shift(out2, PAIR, 1)
    near1, near3 = keep(order[3:5], [[], []])
    got1, got3 = shift(near1, RING, 1), shift(near3, RING, 3)
    in2, far_momenta = lax.optimization_barrier((in2, far_momenta))
    across, opposite = keep(order[5:7], [[in1, in3], [in2]])
    got_across, got_opposite = shift(across, PAIR, 1), shift(opposite, RING, 2)
    (own,) = keep(order[7:], [[]])
    mean, mean_half, square = owner_mean([own, got1, got3, got_across, got_opposite], float(replicas))

    means = {(0, 0): mean_half}
    for by in AROUND:
        means[(0, (4 - by) % 4)] = shift(mean_half, RING, by)
    means[(1, 0)] = shift(mean_half, PAIR, 1)
    square = add_over(square, (RING,))
    square = add_over(square, (PAIR, CORE))
    square, means[(1, 0)] = lax.optimization_barrier((square, means[(1, 0)]))
    means[(1, 3)] = shift(means[(1, 0)], RING, 1)
    means[(1, 1)] = shift(means[(1, 0)], RING, 3)
    means[(1, 2)] = shift(means[(0, 2)], PAIR, 1)
    square = add_over(square, FSDP[1:])
    square = add_over(square, FSDP[:1])

    momenta = (near_momenta, far_momenta)
    other_momenta = (shift(near_momenta, CORE, 1), shift(far_momenta, CORE, 1))
    places, mean_list, momenta_list = [], [], []
    for dx, dy in order:
        for dc in range(2):
            places.append((dx, dy, dc))
            mean_list.append((means[(dx, dy)] if dc == 0 else shift(means[(dx, dy)], CORE, 1), 0))
            momenta_list.append(((momenta if dc == 0 else other_momenta)[dx], dy))
    inner_next, momentum_next, outer_next = finish(
        idx, square, float(entries), outer_weights, replica_inner_weight, momentum, mean,
        places, mean_list, momenta_list,
    )
    return (inner_next, momentum_next, outer_next)


def solution(mesh):
    torus = Mesh(
        mesh.devices.reshape(4, 2, 2, 2, 4), ("rep_0", "rep_1", "rep_2", "fsdp_0", "fsdp_1")
    )
    placed = (P(REP, FSDP, None), P(FSDP, None), P(FSDP, REP), P(REP, FSDP, None), P())
    return jax.shard_map(
        per_device,
        mesh=torus,
        in_specs=placed,
        out_specs=(P(REP, FSDP, None), P(FSDP, REP), P(FSDP, REP)),
        check_vma=False,
    )
```
